32 devices in a mesh: px: 4 (over y, x), py: 8 (over z, core).
Axes of the slice: x: 2, y: 2, z: 4, core: 2. Of those that a mesh axis runs over, the one named last changes fastest.
Arguments:
- photons: float32 [1024, 128], P(('px', 'py')), may hold values from 50 to 1000
- halo_cells: int32 [1024, 128], P(('px', 'py')), may hold values from 0 to 1769471
- halo_counts: int32 [1024], P(('px', 'py')), may hold values from 1 to 128
- owners: int32 [1024, 1], P(('px', 'py')), may hold values from 0 to 7; in each aligned block of 32 rows (0 to 31, 32 to 63, ...) at most 4 rows name the same one
- density: float32 [384, 384, 384], P('px', 'py'), may hold values from 0.02 to 50
Outputs:
- fraction: float32 [384, 384, 384], P('px', 'py')
The draws below stay inside these ranges and needn't reach their ends.
Inputs may be any that keep to these rules, and one draw needn't show every extreme that they name: The halos of a block all lie in pencil owners[b] of the block's own slab. Among the 32 blocks of one device no owner appears more than 4 times, a bound that some block reaches. Slots at or past halo_counts[b] are not live and carry arbitrary values. `halo_cells`: A cell index within the owner pencil is (x * 48 + y) * 384 + z with x, y, z local to that pencil.
All inputs are finite; a program needn't handle non-finite values.
Results may differ from the reference program's by a relative error of at most 0.0003.
Values sent between devices are 32-bit elements; how exact they have to be, the bound alone decides.
A program may use at most 192 MiB of HBM per device.

```python
import math
import jax
import jax.numpy as jnp
import numpy as np
from jax import lax

NG = 384
SLOTS = 128
CAP = 4
RADIUS = 20
BLK_DEV = 32
CX = 96
CY = 48
HROWS = 1024
N_PY = 8


def draw_density(key, part):
    subkeys = jax.random.split(jax.random.fold_in(key, 7), 4)
    wave_numbers = jax.random.randint(subkeys[0], (4, 3), 1, 4)
    flip_signs = jax.random.randint(subkeys[1], (4, 3), 0, 2) * 2 - 1
    wave_numbers = wave_numbers * flip_signs
    phases = jax.random.uniform(subkeys[2], (4,), jnp.float32, -jnp.pi, jnp.pi)
    coords = jnp.arange(NG, dtype=jnp.int32)
    smooth = jnp.zeros((NG, NG, NG), jnp.float32)
    for number in range(4):
        along_x = wave_numbers[number, 0] * coords % NG
        along_y = wave_numbers[number, 1] * coords % NG
        along_z = wave_numbers[number, 2] * coords % NG
        total = (along_x[:, None, None] + along_y[None, :, None] + along_z[None, None, :]) % NG
        smooth = smooth + jnp.cos(total.astype(jnp.float32) * (2.0 * jnp.pi / NG) + phases[number])
    smooth = smooth / jnp.sqrt(2.0)
    rough_part = jnp.clip(1.8 * jax.random.normal(subkeys[3], (NG, NG, NG), jnp.float32), -4.0, 4.0) - 1.4
    amplitude = 0.8
    return jnp.clip(jnp.exp(amplitude * smooth + rough_part), 0.02, 50.0).astype(jnp.float32)


def place_ends(result, own_key, smallest, top_value):
    spot = [jax.random.randint(jax.random.fold_in(own_key, axis), (), 0, length) for axis, length in enumerate(result.shape)]
    main_axis = result.shape.index(max(result.shape))
    neighbour = spot[:main_axis] + [(spot[main_axis] + 1) % result.shape[main_axis]] + spot[main_axis + 1:]
    return result.at[tuple(spot)].set(smallest).at[tuple(neighbour)].set(top_value)


def level_of(key, extent, pieces, low, largest):
    factor_of = 1.0
    for axis_at, shards_of in pieces:
        heights = jax.random.uniform(jax.random.fold_in(jax.random.fold_in(key, 6), axis_at), (shards_of,), jnp.float32, low / len(pieces), largest / len(pieces))
        factor_of = factor_of * jnp.repeat(jnp.exp(heights), extent[axis_at] // shards_of).reshape((-1,) + (1,) * (len(extent) - 1 - axis_at))
    return factor_of


def deal_out(stream_key, own, number, rows, amount, top, most, skew):
    sequence = jax.random.permutation(stream_key, amount)
    crowded, usual = shares(amount, rows * top, most, skew, True), shares(amount, rows * top, most, skew, False)
    places = jnp.arange(amount)

    def named(sizes, rotation):
        used = int((sizes > 0).sum())
        fixed = max(1, used // 4)
        passed = fixed + (places - fixed + rotation * (used - fixed)) % max(1, amount - fixed)
        return jnp.zeros((amount,), jnp.int32).at[sequence[jnp.where(places < fixed, places, passed)]].set(jnp.asarray(sizes, jnp.int32))

    sizes = jnp.where(number % 4 == 0, named(crowded, number // 4), named(usual, number - number // 4 - 1))
    mixed = jax.random.permutation(jax.random.fold_in(own, 3), amount)
    giver, receiver = mixed[0:amount // 2 * 2:2], mixed[1:amount // 2 * 2:2]
    margin = jnp.minimum(sizes[giver] - 1, most - sizes[receiver]) // 2
    margin = jnp.where((giver == sequence[0]) | (receiver == sequence[0]) | (sizes[receiver] == 0), 0, jnp.maximum(margin, 0))
    passed = jax.random.randint(jax.random.fold_in(own, 4), (amount // 2,), 0, 1 << 20) % (margin + 1)
    sizes = sizes.at[giver].add(-passed).at[receiver].add(passed)
    items = jnp.searchsorted(jnp.cumsum(sizes), jnp.arange(rows * top), side="right").astype(jnp.int32)
    table = items.reshape(top, rows).T
    table = table[jax.random.permutation(jax.random.fold_in(own, 1), rows)]
    rotation = jax.random.randint(jax.random.fold_in(own, 2), (rows, 1), 0, top)
    return jnp.take_along_axis(table, (jnp.arange(top)[None, :] + rotation) % top, axis=1)


def shares(count, total, reach, slope, full):
    weights = [(1 << 20) // math.isqrt(rank ** slope) + 1 for rank in range(1, count + 1)]
    largest = reach if full else min(reach, max(-(-total // count), total * weights[0] // sum(weights)))
    least = 1 if total - largest >= count - 1 else 0
    counts, spare = [largest] + [least] * (count - 1), total - largest - least * (count - 1)
    while spare > 0:
        free = [i for i in range(1, count) if counts[i] < largest] or [i for i in range(1, count) if counts[i] < reach]
        whole, budget = sum([weights[i] for i in free]), spare
        for i in free:
            extra = min(reach - counts[i], max(1, budget * weights[i] // whole), spare)
            counts[i] = counts[i] + extra
            spare = spare - extra
    return np.array(counts)


def setup_inputs(seed: int = 0) -> dict:
    seeds = jax.random.split(jax.random.key(seed), 6)
    photons = jnp.clip(jnp.exp(math.log(1000.0) - 2.9957323 * jax.random.uniform(seeds[0], (HROWS, SLOTS), jnp.float32) ** level_of(seeds[0], (HROWS, SLOTS), ((0, 32),), -0.2, 0.2)), 50.0, 1000.0)
    halo_cells = place_ends(jax.random.randint(seeds[1], (HROWS, SLOTS), 0, CX * CY * NG), jax.random.fold_in(seeds[1], 1), 0, (CX * CY * NG) - 1).astype(jnp.int32)
    halo_counts = place_ends(jax.random.randint(seeds[2], (HROWS,), 1, SLOTS + 1), jax.random.fold_in(seeds[2], 1), 1, SLOTS).astype(jnp.int32)
    owners_keys = jax.random.split(jax.random.fold_in(seeds[3], 1), HROWS // BLK_DEV)
    owners_turns = jax.random.permutation(jax.random.fold_in(seeds[3], 3), HROWS // BLK_DEV)
    owners = jax.vmap(lambda own, number: deal_out(jax.random.fold_in(seeds[3], 2), own, number, BLK_DEV, N_PY, 1, CAP, 2))(owners_keys, owners_turns).reshape((HROWS, 1))
    density = draw_density(jax.random.fold_in(seeds[5], 71), 0)
    return dict(photons=photons, halo_cells=halo_cells, halo_counts=halo_counts, owners=owners, density=density)


def top_hat(freq_x, freq_y, freq_z):
    radial = jnp.sqrt(freq_x * freq_x + freq_y * freq_y + freq_z * freq_z) * (2.0 * jnp.pi * RADIUS / NG)
    safe = jnp.where(radial > 0, radial, 1.0)
    value = 3.0 * (jnp.sin(safe) - safe * jnp.cos(safe)) / (safe * safe * safe)
    return jnp.where(radial > 0, value, 1.0)

def reference(photons, halo_cells, halo_counts, owners, density):
    row_count = photons.shape[0]
    row_index = jnp.arange(row_count, dtype=jnp.int32)
    slab_index = row_index // (N_PY * BLK_DEV)
    local_x = halo_cells // (CY * NG)
    local_y = halo_cells // NG % CY
    local_z = halo_cells % NG
    global_x = slab_index[:, None] * CX + local_x
    global_y = owners[:, 0:1] * CY + local_y
    flat_index = ((global_x * NG + global_y) * NG + local_z).astype(jnp.int32)
    live_slots = jnp.arange(photons.shape[1], dtype=jnp.int32)[None, :] < halo_counts[:, None]
    weights = jnp.where(live_slots, photons, jnp.zeros_like(photons))
    field = jnp.zeros((NG * NG * NG,), photons.dtype).at[flat_index.reshape(-1)].add(weights.reshape(-1))
    field = field.reshape(NG, NG, NG)
    packed = lax.complex(field, density)
    spectrum = jnp.fft.fftn(packed)
    index_values = jnp.arange(NG, dtype=jnp.int32)
    signed_frequency = jnp.where(index_values < NG // 2, index_values, index_values - NG).astype(density.dtype)
    window = top_hat(signed_frequency[:, None, None], signed_frequency[None, :, None], signed_frequency[None, None, :])
    smoothed = jnp.fft.ifftn(spectrum * window)
    photon_smooth = jnp.real(smoothed)
    density_smooth = jnp.imag(smoothed)
    fraction = jnp.clip(photon_smooth / jnp.maximum(density_smooth, 0.5), 0.0, 1.0)
    return fraction.astype(jnp.float32)
```

```python
import jax
import jax.numpy as jnp
import numpy as np
from jax import lax
from jax.sharding import PartitionSpec as P

CAP = 4
RADIUS = 20


def product(form, left, right):
    return jnp.einsum(form, left, right, precision=lax.Precision.HIGH)


def hartley(length):
    index_row = np.arange(length)
    angle = (index_row[:, None] * index_row[None, :] % length) * (2.0 * np.pi / length)
    return ((np.cos(angle) + np.sin(angle)) / np.sqrt(length)).astype(np.float32)


def top_hat(freq_x, freq_y, freq_z, grid):
    radial = jnp.sqrt(freq_x * freq_x + freq_y * freq_y + freq_z * freq_z) * (
        2.0 * jnp.pi * RADIUS / grid
    )
    safe = jnp.where(radial > 0, radial, 1.0)
    value = 3.0 * (jnp.sin(safe) - safe * jnp.cos(safe)) / (safe * safe * safe)
    return jnp.where(radial > 0, value, 1.0)


def on_device(photons, halo_cells, halo_counts, owners, density):
    rows_x, rows_y, grid = density.shape
    slots = photons.shape[1]
    count_x = lax.axis_size("px")
    count_y = lax.axis_size("py")
    place_y = lax.axis_index("py")
    devices_all = count_x * count_y
    planes = grid // devices_all
    area = rows_x * rows_y
    table = jnp.asarray(hartley(grid))
    table_x = table.reshape(count_x, rows_x, grid)
    table_y = table.reshape(count_y, rows_y, grid)

    def signed(index_values):
        return jnp.where(index_values < grid // 2, index_values, index_values - grid).astype(
            jnp.float32
        )

    freq = signed(jnp.arange(grid, dtype=jnp.int32))
    freq_z = signed(
        lax.axis_index(("px", "py")) * planes + jnp.arange(planes, dtype=jnp.int32)
    )
    window = top_hat(freq_z[:, None, None], freq[None, :, None], freq[None, None, :], grid)

    def smooth(field_rows):
        spec = product("az,zk->ka", field_rows, table)
        got = lax.all_to_all(
            spec.reshape(devices_all, planes, area),
            ("px", "py"), split_axis=0, concat_axis=0, tiled=True,
        )
        got = got.reshape(count_x, count_y, planes, rows_y, rows_x)
        half = product("iqklx,ixn->qkln", got, table_x)
        full = product("qkln,qlm->kmn", half, table_y) * window
        half = product("kmn,qlm->qkln", full, table_y)
        back = product("qkln,ixn->iqklx", half, table_x)
        got = lax.all_to_all(
            back.reshape(devices_all, planes, area),
            ("px", "py"), split_axis=0, concat_axis=0, tiled=True,
        )
        return product("ka,kz->az", got.reshape(grid, area), table)

    density_rows = density.transpose(1, 0, 2).reshape(area, grid)
    density_smooth = smooth(density_rows)

    slot_index = jnp.arange(slots, dtype=jnp.int32)[None, :]
    weights = jnp.where(slot_index < halo_counts[:, None], photons, 0.0)
    all_weights = lax.all_gather(weights, "py", axis=0, tiled=True)
    all_cells = lax.all_gather(halo_cells, "py", axis=0, tiled=True)
    all_owners = lax.all_gather(owners, "py", axis=0, tiled=True)[:, 0]
    owned = all_owners == place_y
    chosen = jnp.argsort(jnp.where(owned, 0, 1), stable=True)[: CAP * count_y]
    own_weights = jnp.where(owned[chosen][:, None], all_weights[chosen], 0.0)
    own_cells = all_cells[chosen]
    row = own_cells // grid
    spot = ((row % rows_y) * rows_x + row // rows_y) * grid + own_cells % grid
    painted = jnp.zeros((area * grid,), jnp.float32)
    painted = painted.at[spot.reshape(-1)].add(own_weights.reshape(-1))
    photon_smooth = smooth(painted.reshape(area, grid))

    fraction = jnp.clip(photon_smooth / jnp.maximum(density_smooth, 0.5), 0.0, 1.0)
    return fraction.reshape(rows_y, rows_x, grid).transpose(1, 0, 2)


def solution(mesh):
    placed = (
        P(("px", "py"), None),
        P(("px", "py"), None),
        P(("px", "py")),
        P(("px", "py"), None),
        P("px", "py", None),
    )
    return jax.shard_map(
        on_device, mesh=mesh, in_specs=placed, out_specs=P("px", "py", None), check_vma=False
    )
```
